32 devices in a mesh: heads: 4 (over y, core), tokens: 4 (over z), cols: 2 (over x).
Axes of the slice: x: 2, y: 2, z: 4, core: 2. Of those that a mesh axis runs over, the one named last changes fastest.
Arguments:
- query_in: bfloat16 [2048, 8192], P('tokens', ('heads', 'cols')), may hold values from -24 to 24
- key_in: bfloat16 [2048, 8192], P('tokens', ('heads', 'cols')), may hold values from -24 to 24
- value_in: bfloat16 [2048, 8192], P('tokens', ('heads', 'cols')), may hold values from -6 to 6
- out_grads: bfloat16 [2048, 8192], P('tokens', ('heads', 'cols')), may hold values from -6 to 6
- doc_starts: int32 [6], replicated, may hold values from 0 to 2047, as said below
Outputs:
- input_factor: float32 [8192, 8192], P('heads', ('tokens', 'cols'))
- grad_factor: float32 [8192, 8192], P('heads', ('tokens', 'cols'))
The draws below stay inside these ranges and needn't reach their ends.
Inputs may be any that keep to these rules, and one draw needn't show every extreme that they name: Strictly increasing with the first entry 0; document d runs from doc_starts[d] to the next start (the last one to 2048) - 1. One document holds (4 // 2 + 1) * 512 tokens.
All inputs are finite; a program needn't handle non-finite values.
Results may differ from the reference program's by a relative error of at most 0.0041.
Values may be sent and summed in bfloat16 or wider, within the bound.
A program may use at most 128 MiB of HBM per device.

```python
import math
import jax
import jax.numpy as jnp
from jax import lax

HEAD_DIM = 128
TOK_DEV = 512
DOCS = 6
D = 8192
TOKENS = 2048


def cut_points(key):
    long_len = (TOKENS // TOK_DEV // 2 + 1) * TOK_DEV
    rest_len = TOKENS - long_len
    cut_picks = jax.random.permutation(jax.random.fold_in(key, 11), rest_len - 1)[:DOCS - 2] + 1
    bounds = jnp.concatenate([jnp.zeros((1,), jnp.int32), jnp.sort(cut_picks).astype(jnp.int32), jnp.full((1,), rest_len, jnp.int32)])
    others = bounds[1:] - bounds[:-1]
    long_slot = jax.random.randint(jax.random.fold_in(key, 13), (), 0, DOCS).astype(jnp.int32)
    slots = jnp.arange(DOCS, dtype=jnp.int32)
    other_index = jnp.clip(slots - (slots > long_slot).astype(jnp.int32), 0, DOCS - 2)
    doc_lengths = jnp.where(slots == long_slot, long_len, others[other_index]).astype(jnp.int32)
    return jnp.concatenate([jnp.zeros((1,), jnp.int32), jnp.cumsum(doc_lengths)[:-1].astype(jnp.int32)])


def draw_doc_starts(key, part):
    return cut_points(key)


def background(key, salt):
    return jnp.clip(jax.random.normal(jax.random.fold_in(key, salt), (TOKENS, D), jnp.float32), -4.0, 4.0)


def draw_key_in(key, part):
    result = background(key, 31)
    return result.astype(jnp.bfloat16)


def draw_query_in(key, part):
    result = background(key, 37)
    return result.astype(jnp.bfloat16)


def shard_levels(stream_key, extent, cuts, smallest, largest):
    def one(axis_at, blocks):
        draws = jax.random.uniform(jax.random.fold_in(jax.random.fold_in(stream_key, 6), axis_at), (blocks,), jnp.float32, smallest / len(cuts), largest / len(cuts))
        return jnp.repeat(jnp.exp(draws), extent[axis_at] // blocks).reshape((-1,) + (1,) * (len(extent) - axis_at - 1))

    loudness = one(*cuts[0])
    for cut in cuts[1:]:
        loudness = loudness * one(*cut)
    return loudness


def gaussian(own_key, shape, scale, limit, shards=(), kind=jnp.bfloat16):
    factor_of = shard_levels(own_key, shape, shards, -0.22, 0.18) if shards else 1.0
    values = jax.random.normal(own_key, shape, jnp.float32) * scale * factor_of
    return jnp.minimum(jnp.maximum(values, -limit), limit).astype(kind)


def setup_inputs(seed: int = 0) -> dict:
    seeds = jax.random.split(jax.random.key(seed), 6)
    return {
        "query_in": draw_query_in(jax.random.fold_in(seeds[5], 71), 0),
        "key_in": draw_key_in(jax.random.fold_in(seeds[5], 71), 0),
        "value_in": gaussian(seeds[2], (TOKENS, D), 1.0, 6.0, ((0, 4), (1, 8))),
        "out_grads": gaussian(seeds[3], (TOKENS, D), 1.0, 6.0, ((0, 4), (1, 8))),
        "doc_starts": draw_doc_starts(jax.random.fold_in(seeds[5], 71), 0),
    }


MASK_FLOOR = -1e+30

def document_ids(positions, doc_starts):
    return lax.optimization_barrier(jnp.sum((positions[:, None] >= doc_starts[None, :]).astype(jnp.int32), axis=1)) - 1

def reference(query_in, key_in, value_in, out_grads, doc_starts):
    all_tokens, row_width = query_in.shape
    head_count = row_width // HEAD_DIM
    positions = jnp.arange(all_tokens, dtype=jnp.int32)
    doc_ids = document_ids(positions, doc_starts)
    allowed = doc_ids[:, None] == doc_ids[None, :]
    score_scale = 1.0 / math.sqrt(HEAD_DIM)

    def per_head(head_index):
        col_begin = (head_index * HEAD_DIM).astype(jnp.int32)

        def select_cols(source):
            return lax.dynamic_slice_in_dim(source, col_begin, HEAD_DIM, 1).astype(jnp.float32)
        scores = jnp.dot(select_cols(query_in), select_cols(key_in).T, precision=lax.Precision.HIGHEST) * score_scale
        masked = jnp.where(allowed, scores, MASK_FLOOR)
        row_peak = lax.optimization_barrier(jnp.max(masked, axis=1))
        row_mass = lax.optimization_barrier(jnp.sum(jnp.where(allowed, jnp.exp(masked - row_peak[:, None]), 0.0), axis=1))
        log_total = row_peak + jnp.log(row_mass)
        weights = jnp.where(allowed, jnp.exp(scores - log_total[:, None]), 0.0).astype(jnp.bfloat16)
        weights = lax.optimization_barrier(weights).astype(jnp.float32)
        attended = jnp.dot(weights, select_cols(value_in), precision=lax.Precision.HIGHEST)
        grad_rows = jnp.dot(weights.T, select_cols(out_grads), precision=lax.Precision.HIGHEST)
        return (attended, grad_rows)
    attended, grad_rows = lax.map(per_head, jnp.arange(head_count, dtype=jnp.int32))
    attended = attended.transpose(1, 0, 2).reshape(all_tokens, row_width).astype(jnp.bfloat16)
    value_grads = grad_rows.transpose(1, 0, 2).reshape(all_tokens, row_width).astype(jnp.bfloat16)
    attended_wide = attended.astype(jnp.float32)
    grads_wide = value_grads.astype(jnp.float32)
    input_factor = jnp.dot(attended_wide.T, attended_wide, precision=lax.Precision.HIGHEST) / all_tokens
    grad_factor = jnp.dot(grads_wide.T, grads_wide, precision=lax.Precision.HIGHEST) / all_tokens
    return (input_factor, grad_factor)
```

```python
import math

import jax
import jax.numpy as jnp
from jax import lax
from jax.experimental import pallas as pl
from jax.experimental.pallas import tpu as pltpu
from jax.sharding import PartitionSpec as P

HEAD_DIM = 128


MASK_FLOOR = -1e30


def spread(value, axis, source):
    kept = jnp.where(lax.axis_index(axis) == source, value, 0).astype(value.dtype)
    return lax.psum(kept, axis)


def document_ids(positions, doc_starts):
    return jnp.sum((positions[:, None] >= doc_starts[None, :]).astype(jnp.int32), axis=1) - 1


def pair_scores(query_rows, key_rows, query_pos, key_pos, doc_starts):
    head_count = query_rows.shape[1] // HEAD_DIM
    query_heads = query_rows.reshape(query_rows.shape[0], head_count, HEAD_DIM)
    key_heads = key_rows.reshape(key_rows.shape[0], head_count, HEAD_DIM)
    scores = jnp.einsum(
        "qhd,khd->hqk", query_heads, key_heads, preferred_element_type=jnp.float32
    ) * (1.0 / math.sqrt(HEAD_DIM))
    query_docs = document_ids(query_pos, doc_starts)
    key_docs = document_ids(key_pos, doc_starts)
    allowed = query_docs[:, None] == key_docs[None, :]
    return (scores, allowed[None, :, :])


def on_device(query_in, key_in, value_in, out_grads, doc_starts):
    tok_dev, row_width = query_in.shape
    head_count = row_width // HEAD_DIM
    first_pos = lax.axis_index("tokens") * tok_dev
    query_pos = first_pos + jnp.arange(tok_dev, dtype=jnp.int32)
    keys_all, values_all = (
        lax.all_gather(key_in, "tokens", axis=0, tiled=True),
        lax.all_gather(value_in, "tokens", axis=0, tiled=True),
    )
    all_tokens = keys_all.shape[0]
    key_span = min(512, all_tokens)
    block_ids = jnp.arange(all_tokens // key_span, dtype=jnp.int32)

    def block_scores(block_id):
        key_begin = block_id * key_span
        key_rows = lax.dynamic_slice_in_dim(keys_all, key_begin, key_span, 0)
        key_pos = key_begin + jnp.arange(key_span, dtype=jnp.int32)
        scores, allowed = pair_scores(query_in, key_rows, query_pos, key_pos, doc_starts)
        return (key_begin, scores, allowed)

    def gated(block_id, update, running):
        key_begin = block_id * key_span
        return update(running)

    def stats_step(running, block_id):

        def update(state):
            row_peak, row_mass = state
            key_begin, scores, allowed = block_scores(block_id)
            masked = jnp.where(allowed, scores, MASK_FLOOR)
            new_peak = jnp.maximum(row_peak, jnp.max(masked, axis=2))
            new_mass = row_mass * jnp.exp(row_peak - new_peak) + jnp.sum(
                jnp.where(allowed, jnp.exp(masked - new_peak[:, :, None]), 0.0), axis=2
            )
            return (new_peak, new_mass)

        return (gated(block_id, update, running), None)

    initial = (
        jnp.full((head_count, tok_dev), MASK_FLOOR, jnp.float32),
        jnp.zeros((head_count, tok_dev), jnp.float32),
    )
    (row_peak, row_mass), _ = lax.scan(stats_step, initial, block_ids)
    log_total = row_peak + jnp.log(row_mass)

    def value_step(running, block_id):

        def update(state):
            weighted, partials = state
            key_begin, scores, allowed = block_scores(block_id)
            weights = jnp.where(allowed, jnp.exp(scores - log_total[:, :, None]), 0.0).astype(
                jnp.bfloat16
            )
            value_rows = lax.dynamic_slice_in_dim(values_all, key_begin, key_span, 0).reshape(
                key_span, head_count, HEAD_DIM
            )
            weighted = weighted + jnp.einsum(
                "hqk,khd->qhd", weights, value_rows, preferred_element_type=jnp.float32
            )
            return (weighted, partials)

        return (gated(block_id, update, running), None)

    partial_rows = 8
    value_init = (
        jnp.zeros((tok_dev, head_count, HEAD_DIM), jnp.float32),
        jnp.zeros((partial_rows, row_width), jnp.float32),
    )
    (weighted, partials), _ = lax.scan(value_step, value_init, block_ids)
    attended = weighted.reshape(tok_dev, row_width).astype(jnp.bfloat16)
    stats_all = lax.all_gather(log_total.T, "tokens", axis=0, tiled=True)
    query_rows = lax.all_gather(query_in, "tokens", axis=0, tiled=True)
    grad_rows = lax.all_gather(out_grads, "tokens", axis=0, tiled=True)
    piece_rows = query_rows.shape[0]
    piece_pos = jnp.arange(piece_rows, dtype=jnp.int32)

    def update(grad_sum):
        scores, allowed = pair_scores(query_rows, key_in, piece_pos, query_pos, doc_starts)
        weights = jnp.where(allowed, jnp.exp(scores - stats_all.T[:, :, None]), 0.0).astype(
            jnp.bfloat16
        )
        piece_grads = grad_rows.reshape(piece_rows, head_count, HEAD_DIM)
        return jnp.einsum("hqk,qhd->khd", weights, piece_grads, preferred_element_type=jnp.float32)

    summed = update(jnp.zeros((tok_dev, head_count, HEAD_DIM), jnp.float32))
    value_grads = summed.reshape(tok_dev, row_width).astype(jnp.bfloat16)
    token_shards = lax.axis_size("tokens")
    col_shards = lax.axis_size("cols")
    rows_attended, rows_grads = (
        lax.all_gather(attended[None], ("tokens", "cols"), axis=0, tiled=True),
        lax.all_gather(value_grads[None], ("tokens", "cols"), axis=0, tiled=True),
    )
    rows_attended = rows_attended.reshape(token_shards, col_shards, tok_dev, row_width)
    rows_grads = rows_grads.reshape(token_shards, col_shards, tok_dev, row_width)
    own_attended = lax.dynamic_index_in_dim(
        rows_attended, lax.axis_index("cols"), 1, keepdims=False
    )
    own_grads = lax.dynamic_index_in_dim(rows_grads, lax.axis_index("cols"), 1, keepdims=False)
    cols_attended, cols_grads = (
        spread(own_attended, "heads", lax.axis_index("tokens")),
        spread(own_grads, "heads", lax.axis_index("tokens")),
    )
    input_factor = jnp.einsum(
        "acnf,ang->cfg", rows_attended, cols_attended, preferred_element_type=jnp.float32
    )
    grad_factor = jnp.einsum(
        "acnf,ang->cfg", rows_grads, cols_grads, preferred_element_type=jnp.float32
    )
    input_factor = input_factor.reshape(col_shards * row_width, row_width) / all_tokens
    grad_factor = grad_factor.reshape(col_shards * row_width, row_width) / all_tokens
    return (input_factor, grad_factor)


BLOCK_Q = 256
F32 = jnp.float32
BF16 = jnp.bfloat16


def fused_kernel(
    q_ref, k_ref, v_ref, g_ref, dk_ref, dq_ref, out_a, out_g,
    xin, rows, cols, v_t, g_acc, stage,
    own_sem, a2a_send, a2a_recv, row_recv, x_send, up_send, down_send,
    col_recv, pair_send, y_send, relay_send, out_sem,
):
    n = lax.axis_size("tokens")
    tok_dev = q_ref.shape[0]
    all_tokens = n * tok_dev
    h = lax.axis_index("heads")
    z = lax.axis_index("tokens")
    x = lax.axis_index("cols")
    y = h // 2
    core = h % 2
    other_x = 1 - x
    pair = y * 2 + (1 - core)
    inputs = (q_ref, k_ref, v_ref, g_ref)

    barrier = pltpu.get_barrier_semaphore()
    for step in range(1, n):
        pl.semaphore_signal(barrier, inc=1, device_id={"tokens": (z + step) % n})
    for step in range(1, 4):
        pl.semaphore_signal(barrier, inc=1, device_id={"heads": (h + step) % 4})
    pl.semaphore_signal(barrier, inc=1, device_id={"cols": other_x})
    pl.semaphore_wait(barrier, n + 3)

    def a2a_copy(j, a, step):
        target = (z + step) % n
        return pltpu.make_async_remote_copy(
            src_ref=inputs[a].at[:, pl.ds(pl.multiple_of((j * n + target) * 128, 128), 128)],
            dst_ref=xin.at[j, a, pl.ds(pl.multiple_of(z * tok_dev, tok_dev), tok_dev), :],
            send_sem=a2a_send.at[j, a, step],
            recv_sem=a2a_recv.at[j, a, step],
            device_id={"tokens": target},
        )

    def own_copy(j, a):
        return pltpu.make_async_copy(
            inputs[a].at[:, pl.ds(pl.multiple_of((j * n + z) * 128, 128), 128)],
            xin.at[j, a, pl.ds(pl.multiple_of(z * tok_dev, tok_dev), tok_dev), :],
            own_sem.at[j, a],
        )

    for j in range(2):
        for a in range(4):
            for step in (2, 1, 3):
                a2a_copy(j, a, step).start()
            own_copy(j, a).start()

    def attention(j):
        for a in range(4):
            own_copy(j, a).wait()
            for step in range(1, n):
                a2a_copy(j, a, step).wait()
        v_t[...] = xin[j, 2].astype(F32).T.astype(BF16)
        g_acc[...] = jnp.zeros_like(g_acc)

        def block(ib, carry):
            span = pl.ds(pl.multiple_of(ib * BLOCK_Q, BLOCK_Q), BLOCK_Q)
            s = lax.dot_general(
                xin[j, 1], xin[j, 0, span, :], (((1,), (1,)), ((), ())),
                preferred_element_type=F32,
            ) * (1.0 / math.sqrt(HEAD_DIM))
            s = jnp.where(dk_ref[...] == dq_ref[:, span], s, MASK_FLOOR)
            e = jnp.exp(s - jnp.max(s, axis=0, keepdims=True))
            p = (e * (1.0 / jnp.sum(e, axis=0, keepdims=True))).astype(BF16)
            att = jnp.dot(v_t[...], p, preferred_element_type=F32)
            rows[j, 0, x, z, :, span] = att.astype(BF16)
            g_acc[...] += jnp.dot(p, xin[j, 3, span, :], preferred_element_type=F32)
            return carry

        lax.fori_loop(0, all_tokens // BLOCK_Q, block, 0)
        rows[j, 1, x, z] = g_acc[...].T.astype(BF16)

    def row_copy(j, f, xs, zs, send, device):
        piece = rows.at[j, f, xs, zs]
        return pltpu.make_async_remote_copy(
            src_ref=piece, dst_ref=piece, send_sem=send.at[j, f, zs],
            recv_sem=row_recv.at[j, f, xs, zs], device_id=device,
        )

    def x_copy(j, f, zs):
        return row_copy(j, f, x, zs, x_send, {"cols": other_x})

    def up_copy(j, f, zs):
        return row_copy(j, f, x, zs, up_send, {"tokens": (z + 1) % n})

    def down_copy(j, f, zs):
        return row_copy(j, f, x, zs, down_send, {"tokens": (z + n - 1) % n})

    def col_copy(j, f, zs, source, send, device):
        return pltpu.make_async_remote_copy(
            src_ref=source, dst_ref=cols.at[j, f, zs], send_sem=send.at[j, f, zs],
            recv_sem=col_recv.at[j, f, zs], device_id={"heads": device},
        )

    def pair_copy(j, f, zs):
        return col_copy(j, f, zs, rows.at[j, f, x, zs], pair_send, pair)

    def y_copy(j, f, zs):
        return col_copy(j, f, zs, rows.at[j, f, x, zs], y_send, (1 - y) * 2 + zs % 2)

    def relay_copy(j, f, zs):
        return col_copy(j, f, zs, cols.at[j, f, zs], relay_send, pair)

    is_source = h == z
    far = y != z // 2

    def feed_cols(j, f, zs):
        @pl.when(is_source)
        def _():
            pair_copy(j, f, zs).start()
            y_copy(j, f, zs).start()

    def send_own(j, f):
        @pl.when(z < n - 1)
        def _():
            up_copy(j, f, z).start()

        @pl.when(z > 0)
        def _():
            down_copy(j, f, z).start()

        x_copy(j, f, z).start()
        feed_cols(j, f, z)

    def relay_step(j, f, step):
        @pl.when(z >= step)
        def _():
            zs = z - step
            x_copy(j, f, zs).wait_recv()

            @pl.when(z < n - 1)
            def _():
                up_copy(j, f, zs).start()

            x_copy(j, f, zs).start()
            feed_cols(j, f, zs)

        @pl.when(z + step < n)
        def _():
            zs = z + step
            x_copy(j, f, zs).wait_recv()

            @pl.when(z > 0)
            def _():
                down_copy(j, f, zs).start()

            x_copy(j, f, zs).start()
            feed_cols(j, f, zs)

    def relay_cols(j, f):
        for zs in range(n):
            @pl.when(far & (core == zs % 2))
            def _():
                relay_copy(j, f, zs).wait_recv()
                relay_copy(j, f, zs).start()

    def finish(j, f):
        def one(zs, carry):
            row_copy(j, f, other_x, zs, x_send, {"cols": other_x}).wait_recv()
            return carry

        lax.fori_loop(0, n, one, 0)
        for zs in range(n):
            @pl.when((h != z) & jnp.logical_not(far & (core == zs % 2)))
            def _():
                relay_copy(j, f, zs).wait_recv()

        @pl.when(is_source)
        def _():
            def move(zs, carry):
                cols[j, f, zs] = rows[j, f, x, zs]
                return carry

            lax.fori_loop(0, n, move, 0)

    used = [0]
    span_rows = n * 128

    def out_copy(f, xs, jr, jc, slot):
        target = (out_a, out_g)[f]
        return pltpu.make_async_copy(
            stage.at[slot],
            target.at[
                pl.ds(pl.multiple_of(xs * (2 * span_rows) + jr * span_rows, span_rows), span_rows),
                pl.ds(jc * span_rows, span_rows),
            ],
            out_sem.at[slot],
        )

    def tiles(f, xs, jr, jc):
        slot = used[0] % 2
        if used[0] >= 2:
            out_copy(f, xs, jr, jc, slot).wait()
        used[0] += 1

        def part(m, carry):
            left = rows[jr, f, xs, pl.ds(2 * m, 2)].reshape(256, all_tokens)
            right = cols[jc, f].reshape(span_rows, all_tokens)
            stage[slot, pl.ds(pl.multiple_of(m * 256, 256), 256), :] = lax.dot_general(
                left, right, (((1,), (1,)), ((), ())), preferred_element_type=F32
            ) * (1.0 / all_tokens)
            return carry

        lax.fori_loop(0, n // 2, part, 0)
        out_copy(f, xs, jr, jc, slot).start()

    attention(0)
    send_own(0, 0)
    send_own(0, 1)
    attention(1)
    send_own(1, 0)
    send_own(1, 1)
    for f in range(2):
        for step in range(1, n):
            relay_step(0, f, step)
        relay_cols(0, f)
    for step in range(1, n):
        relay_step(1, 0, step)
    relay_cols(1, 0)
    early = []
    for f in range(2):
        early += [(f, x, 0, 0), (f, other_x, 0, 0)]
    finish(0, 0)
    finish(0, 1)
    for step in range(1, n):
        relay_step(1, 1, step)
        if step < n:
            tiles(*early[step - 1])
    relay_cols(1, 1)
    for item in early[n - 1:]:
        tiles(*item)
    for f in range(2):
        finish(1, f)
        for xs in (x, other_x):
            for jr, jc in ((0, 1), (1, 0), (1, 1)):
                tiles(f, xs, jr, jc)
    for slot in range(2):
        out_copy(0, x, 0, 0, slot).wait()

    for j in range(2):
        for f in range(2):
            for zs in range(n):
                x_copy(j, f, zs).wait_send()

                @pl.when((z < n - 1) & (zs <= z))
                def _():
                    up_copy(j, f, zs).wait_send()

                @pl.when((z > 0) & (zs >= z))
                def _():
                    down_copy(j, f, zs).wait_send()

                @pl.when(is_source)
                def _():
                    pair_copy(j, f, zs).wait_send()
                    y_copy(j, f, zs).wait_send()

                @pl.when(far & (core == zs % 2))
                def _():
                    relay_copy(j, f, zs).wait_send()


def fused(query_in, key_in, value_in, out_grads, doc_starts):
    n = lax.axis_size("tokens")
    tok_dev, row_width = query_in.shape
    all_tokens = n * tok_dev
    docs = document_ids(jnp.arange(all_tokens, dtype=jnp.int32), doc_starts)
    dma = pltpu.SemaphoreType.DMA
    hbm = pl.BlockSpec(memory_space=pl.ANY)
    vmem = pl.BlockSpec(memory_space=pltpu.VMEM)
    out = jax.ShapeDtypeStruct((2 * row_width, row_width), F32)
    return tuple(pl.pallas_call(
        fused_kernel,
        out_shape=(out, out),
        in_specs=[hbm] * 4 + [vmem] * 2,
        out_specs=[hbm] * 2,
        scratch_shapes=[
            pltpu.VMEM((2, 4, all_tokens, HEAD_DIM), BF16),
            pltpu.VMEM((2, 2, 2, n, HEAD_DIM, all_tokens), BF16),
            pltpu.VMEM((2, 2, n, HEAD_DIM, all_tokens), BF16),
            pltpu.VMEM((HEAD_DIM, all_tokens), BF16),
            pltpu.VMEM((all_tokens, HEAD_DIM), F32),
            pltpu.VMEM((2, n * HEAD_DIM, n * HEAD_DIM), F32),
            dma((2, 4)), dma((2, 4, n)), dma((2, 4, n)),
            dma((2, 2, 2, n)), dma((2, 2, n)), dma((2, 2, n)), dma((2, 2, n)),
            dma((2, 2, n)), dma((2, 2, n)), dma((2, 2, n)), dma((2, 2, n)),
            dma((2,)),
        ],
        compiler_params=pltpu.CompilerParams(
            collective_id=0, has_side_effects=True, vmem_limit_bytes=60 * 1024 * 1024
        ),
    )(query_in, key_in, value_in, out_grads, docs[:, None], docs[None, :]))


def per_device(query_in, key_in, value_in, out_grads, doc_starts):
    n = lax.axis_size("tokens")
    fits = n == 4 and lax.axis_size("heads") == 4 and lax.axis_size("cols") == 2
    if fits and query_in.shape[1] == 2 * n * HEAD_DIM and query_in.shape[0] % BLOCK_Q == 0:
        return fused(query_in, key_in, value_in, out_grads, doc_starts)
    return on_device(query_in, key_in, value_in, out_grads, doc_starts)


def solution(mesh):
    in_specs = (
        P("tokens", ("heads", "cols")),
        P("tokens", ("heads", "cols")),
        P("tokens", ("heads", "cols")),
        P("tokens", ("heads", "cols")),
        P(),
    )
    out_specs = (P("heads", ("tokens", "cols")), P("heads", ("tokens", "cols")))
    return jax.shard_map(
        per_device, mesh=mesh, in_specs=in_specs, out_specs=out_specs, check_vma=False
    )
```

```python
import math

import jax
import jax.numpy as jnp
from jax import lax
from jax.experimental import pallas as pl
from jax.experimental.pallas import tpu as pltpu
from jax.sharding import PartitionSpec as P

HEAD_DIM = 128


MASK_FLOOR = -1e30


def spread(value, axis, source):
    kept = jnp.where(lax.axis_index(axis) == source, value, 0).astype(value.dtype)
    return lax.psum(kept, axis)


def document_ids(positions, doc_starts):
    return jnp.sum((positions[:, None] >= doc_starts[None, :]).astype(jnp.int32), axis=1) - 1


def pair_scores(query_rows, key_rows, query_pos, key_pos, doc_starts):
    head_count = query_rows.shape[1] // HEAD_DIM
    query_heads = query_rows.reshape(query_rows.shape[0], head_count, HEAD_DIM)
    key_heads = key_rows.reshape(key_rows.shape[0], head_count, HEAD_DIM)
    scores = jnp.einsum(
        "qhd,khd->hqk", query_heads, key_heads, preferred_element_type=jnp.float32
    ) * (1.0 / math.sqrt(HEAD_DIM))
    query_docs = document_ids(query_pos, doc_starts)
    key_docs = document_ids(key_pos, doc_starts)
    allowed = query_docs[:, None] == key_docs[None, :]
    return (scores, allowed[None, :, :])


def on_device(query_in, key_in, value_in, out_grads, doc_starts):
    tok_dev, row_width = query_in.shape
    head_count = row_width // HEAD_DIM
    first_pos = lax.axis_index("tokens") * tok_dev
    query_pos = first_pos + jnp.arange(tok_dev, dtype=jnp.int32)
    keys_all, values_all = (
        lax.all_gather(key_in, "tokens", axis=0, tiled=True),
        lax.all_gather(value_in, "tokens", axis=0, tiled=True),
    )
    all_tokens = keys_all.shape[0]
    key_span = min(512, all_tokens)
    block_ids = jnp.arange(all_tokens // key_span, dtype=jnp.int32)

    def block_scores(block_id):
        key_begin = block_id * key_span
        key_rows = lax.dynamic_slice_in_dim(keys_all, key_begin, key_span, 0)
        key_pos = key_begin + jnp.arange(key_span, dtype=jnp.int32)
        scores, allowed = pair_scores(query_in, key_rows, query_pos, key_pos, doc_starts)
        return (key_begin, scores, allowed)

    def gated(block_id, update, running):
        key_begin = block_id * key_span
        return update(running)

    def stats_step(running, block_id):

        def update(state):
            row_peak, row_mass = state
            key_begin, scores, allowed = block_scores(block_id)
            masked = jnp.where(allowed, scores, MASK_FLOOR)
            new_peak = jnp.maximum(row_peak, jnp.max(masked, axis=2))
            new_mass = row_mass * jnp.exp(row_peak - new_peak) + jnp.sum(
                jnp.where(allowed, jnp.exp(masked - new_peak[:, :, None]), 0.0), axis=2
            )
            return (new_peak, new_mass)

        return (gated(block_id, update, running), None)

    initial = (
        jnp.full((head_count, tok_dev), MASK_FLOOR, jnp.float32),
        jnp.zeros((head_count, tok_dev), jnp.float32),
    )
    (row_peak, row_mass), _ = lax.scan(stats_step, initial, block_ids)
    log_total = row_peak + jnp.log(row_mass)

    def value_step(running, block_id):

        def update(state):
            weighted, partials = state
            key_begin, scores, allowed = block_scores(block_id)
            weights = jnp.where(allowed, jnp.exp(scores - log_total[:, :, None]), 0.0).astype(
                jnp.bfloat16
            )
            value_rows = lax.dynamic_slice_in_dim(values_all, key_begin, key_span, 0).reshape(
                key_span, head_count, HEAD_DIM
            )
            weighted = weighted + jnp.einsum(
                "hqk,khd->qhd", weights, value_rows, preferred_element_type=jnp.float32
            )
            return (weighted, partials)

        return (gated(block_id, update, running), None)

    partial_rows = 8
    value_init = (
        jnp.zeros((tok_dev, head_count, HEAD_DIM), jnp.float32),
        jnp.zeros((partial_rows, row_width), jnp.float32),
    )
    (weighted, partials), _ = lax.scan(value_step, value_init, block_ids)
    attended = weighted.reshape(tok_dev, row_width).astype(jnp.bfloat16)
    stats_all = lax.all_gather(log_total.T, "tokens", axis=0, tiled=True)
    query_rows = lax.all_gather(query_in, "tokens", axis=0, tiled=True)
    grad_rows = lax.all_gather(out_grads, "tokens", axis=0, tiled=True)
    piece_rows = query_rows.shape[0]
    piece_pos = jnp.arange(piece_rows, dtype=jnp.int32)

    def update(grad_sum):
        scores, allowed = pair_scores(query_rows, key_in, piece_pos, query_pos, doc_starts)
        weights = jnp.where(allowed, jnp.exp(scores - stats_all.T[:, :, None]), 0.0).astype(
            jnp.bfloat16
        )
        piece_grads = grad_rows.reshape(piece_rows, head_count, HEAD_DIM)
        return jnp.einsum("hqk,qhd->khd", weights, piece_grads, preferred_element_type=jnp.float32)

    summed = update(jnp.zeros((tok_dev, head_count, HEAD_DIM), jnp.float32))
    value_grads = summed.reshape(tok_dev, row_width).astype(jnp.bfloat16)
    token_shards = lax.axis_size("tokens")
    col_shards = lax.axis_size("cols")
    rows_attended, rows_grads = (
        lax.all_gather(attended[None], ("tokens", "cols"), axis=0, tiled=True),
        lax.all_gather(value_grads[None], ("tokens", "cols"), axis=0, tiled=True),
    )
    rows_attended = rows_attended.reshape(token_shards, col_shards, tok_dev, row_width)
    rows_grads = rows_grads.reshape(token_shards, col_shards, tok_dev, row_width)
    own_attended = lax.dynamic_index_in_dim(
        rows_attended, lax.axis_index("cols"), 1, keepdims=False
    )
    own_grads = lax.dynamic_index_in_dim(rows_grads, lax.axis_index("cols"), 1, keepdims=False)
    cols_attended, cols_grads = (
        spread(own_attended, "heads", lax.axis_index("tokens")),
        spread(own_grads, "heads", lax.axis_index("tokens")),
    )
    input_factor = jnp.einsum(
        "acnf,ang->cfg", rows_attended, cols_attended, preferred_element_type=jnp.float32
    )
    grad_factor = jnp.einsum(
        "acnf,ang->cfg", rows_grads, cols_grads, preferred_element_type=jnp.float32
    )
    input_factor = input_factor.reshape(col_shards * row_width, row_width) / all_tokens
    grad_factor = grad_factor.reshape(col_shards * row_width, row_width) / all_tokens
    return (input_factor, grad_factor)


BLOCK_Q = 256
SWAPPED = ((0, 1), (1, 0))
F32 = jnp.float32
BF16 = jnp.bfloat16


def fused_kernel(
    q_ref, k_ref, v_ref, g_ref, dk_ref, dq_ref, out_a, out_g,
    xin, rows, cols, v_t, g_acc, stage,
    own_sem, a2a_send, a2a_recv, row_recv, x_send, up_send, down_send,
    col_recv, pair_send, y_send, relay_send, swap_send, out_sem,
):
    n = lax.axis_size("tokens")
    tok_dev = q_ref.shape[0]
    all_tokens = n * tok_dev
    h = lax.axis_index("heads")
    z = lax.axis_index("tokens")
    x = lax.axis_index("cols")
    y = h // 2
    core = h % 2
    other_x = 1 - x
    pair = y * 2 + (1 - core)
    inputs = (q_ref, k_ref, v_ref, g_ref)

    barrier = pltpu.get_barrier_semaphore()
    for step in range(1, n):
        pl.semaphore_signal(barrier, inc=1, device_id={"tokens": (z + step) % n})
    for step in range(1, 4):
        pl.semaphore_signal(barrier, inc=1, device_id={"heads": (h + step) % 4})
    pl.semaphore_signal(barrier, inc=1, device_id={"cols": other_x})
    pl.semaphore_wait(barrier, n + 3)

    def a2a_copy(j, a, step):
        target = (z + step) % n
        return pltpu.make_async_remote_copy(
            src_ref=inputs[a].at[:, pl.ds(pl.multiple_of((j * n + target) * 128, 128), 128)],
            dst_ref=xin.at[j, a, pl.ds(pl.multiple_of(z * tok_dev, tok_dev), tok_dev), :],
            send_sem=a2a_send.at[j, a, step],
            recv_sem=a2a_recv.at[j, a, step],
            device_id={"tokens": target},
        )

    def own_copy(j, a):
        return pltpu.make_async_copy(
            inputs[a].at[:, pl.ds(pl.multiple_of((j * n + z) * 128, 128), 128)],
            xin.at[j, a, pl.ds(pl.multiple_of(z * tok_dev, tok_dev), tok_dev), :],
            own_sem.at[j, a],
        )

    def send_inputs(j):
        for a in range(4):
            for step in (2, 1, 3):
                a2a_copy(j, a, step).start()
            own_copy(j, a).start()

    def attention(j):
        for a in range(4):
            own_copy(j, a).wait()
            for step in range(1, n):
                a2a_copy(j, a, step).wait()
        if j == 0:
            send_inputs(1)
        v_t[...] = xin[j, 2].astype(F32).T.astype(BF16)
        g_acc[...] = jnp.zeros_like(g_acc)

        def block(ib, carry):
            span = pl.ds(pl.multiple_of(ib * BLOCK_Q, BLOCK_Q), BLOCK_Q)
            s = lax.dot_general(
                xin[j, 1], xin[j, 0, span, :], (((1,), (1,)), ((), ())),
                preferred_element_type=F32,
            ) * (1.0 / math.sqrt(HEAD_DIM))
            s = jnp.where(dk_ref[...] == dq_ref[:, span], s, MASK_FLOOR)
            e = jnp.exp(s - jnp.max(s, axis=0, keepdims=True))
            p = (e * (1.0 / jnp.sum(e, axis=0, keepdims=True))).astype(BF16)
            att = jnp.dot(v_t[...], p, preferred_element_type=F32)
            rows[j, 0, x, z, :, span] = att.astype(BF16)
            g_acc[...] += jnp.dot(p, xin[j, 3, span, :], preferred_element_type=F32)
            return carry

        lax.fori_loop(0, all_tokens // BLOCK_Q, block, 0)
        rows[j, 1, x, z] = g_acc[...].T.astype(BF16)

    def row_copy(j, f, xs, zs, send, device):
        piece = rows.at[j, f, xs, zs]
        return pltpu.make_async_remote_copy(
            src_ref=piece, dst_ref=piece, send_sem=send.at[j, f, zs],
            recv_sem=row_recv.at[j, f, xs, zs], device_id=device,
        )

    def x_copy(j, f, zs):
        return row_copy(j, f, x, zs, x_send, {"cols": other_x})

    def up_copy(j, f, zs):
        return row_copy(j, f, x, zs, up_send, {"tokens": (z + 1) % n})

    def down_copy(j, f, zs):
        return row_copy(j, f, x, zs, down_send, {"tokens": (z + n - 1) % n})

    def col_copy(j, f, zs, source, send, device):
        return pltpu.make_async_remote_copy(
            src_ref=source, dst_ref=cols.at[j, f, zs], send_sem=send.at[j, f, zs],
            recv_sem=col_recv.at[j, f, zs], device_id={"heads": device},
        )

    def pair_copy(j, f, zs):
        return col_copy(j, f, zs, rows.at[j, f, x, zs], pair_send, pair)

    def y_copy(j, f, zs):
        return col_copy(j, f, zs, rows.at[j, f, x, zs], y_send, (1 - y) * 2 + zs % 2)

    def relay_copy(j, f, zs):
        return col_copy(j, f, zs, cols.at[j, f, zs], relay_send, pair)

    mate = z + 1 - 2 * (z % 2)

    def swap_copy(j, f, zs):
        return row_copy(j, f, other_x, zs, swap_send, {"tokens": mate})

    def swap(j, f):
        x_copy_in = row_copy(j, f, other_x, z, x_send, {"cols": other_x})
        x_copy_in.wait_recv()
        swap_copy(j, f, z).start()

    def relay_x(j, f, zs):
        if (j, f) in SWAPPED:
            @pl.when(zs != mate)
            def _():
                x_copy(j, f, zs).start()
        else:
            x_copy(j, f, zs).start()

    is_source = h == z
    far = y != z // 2

    def feed_cols(j, f, zs):
        @pl.when(is_source)
        def _():
            pair_copy(j, f, zs).start()
            y_copy(j, f, zs).start()

    def send_own(j, f):
        @pl.when(z < n - 1)
        def _():
            up_copy(j, f, z).start()

        @pl.when(z > 0)
        def _():
            down_copy(j, f, z).start()

        x_copy(j, f, z).start()
        feed_cols(j, f, z)

    def relay_step(j, f, step):
        @pl.when(z >= step)
        def _():
            zs = z - step
            x_copy(j, f, zs).wait_recv()

            @pl.when(z < n - 1)
            def _():
                up_copy(j, f, zs).start()

            relay_x(j, f, zs)
            feed_cols(j, f, zs)

        @pl.when(z + step < n)
        def _():
            zs = z + step
            x_copy(j, f, zs).wait_recv()

            @pl.when(z > 0)
            def _():
                down_copy(j, f, zs).start()

            relay_x(j, f, zs)
            feed_cols(j, f, zs)

    def relay_cols(j, f):
        for zs in range(n):
            @pl.when(far & (core == zs % 2))
            def _():
                relay_copy(j, f, zs).wait_recv()
                relay_copy(j, f, zs).start()

    def finish_rows(j, f):
        def one(zs, carry):
            waiting = row_copy(j, f, other_x, zs, x_send, {"cols": other_x})
            if (j, f) in SWAPPED:
                @pl.when(zs != z)
                def _():
                    waiting.wait_recv()
            else:
                waiting.wait_recv()
            return carry

        lax.fori_loop(0, n, one, 0)

    def finish_cols(j, f):
        for zs in range(n):
            @pl.when((h != z) & jnp.logical_not(far & (core == zs % 2)))
            def _():
                relay_copy(j, f, zs).wait_recv()

        @pl.when(is_source)
        def _():
            def move(zs, carry):
                cols[j, f, zs] = rows[j, f, x, zs]
                return carry

            lax.fori_loop(0, n, move, 0)

    used = [0]
    span_rows = n * 128

    def out_copy(f, xs, jr, jc, slot):
        target = (out_a, out_g)[f]
        return pltpu.make_async_copy(
            stage.at[slot],
            target.at[
                pl.ds(pl.multiple_of(xs * (2 * span_rows) + jr * span_rows, span_rows), span_rows),
                pl.ds(jc * span_rows, span_rows),
            ],
            out_sem.at[slot],
        )

    def tiles(f, xs, jr, jc):
        slot = used[0] % 2
        if used[0] >= 2:
            out_copy(f, xs, jr, jc, slot).wait()
        used[0] += 1

        def part(m, carry):
            left = rows[jr, f, xs, pl.ds(2 * m, 2)].reshape(256, all_tokens)
            right = cols[jc, f].reshape(span_rows, all_tokens)
            stage[slot, pl.ds(pl.multiple_of(m * 256, 256), 256), :] = lax.dot_general(
                left, right, (((1,), (1,)), ((), ())), preferred_element_type=F32
            ) * (1.0 / all_tokens)
            return carry

        lax.fori_loop(0, n // 2, part, 0)
        out_copy(f, xs, jr, jc, slot).start()

    send_inputs(0)
    attention(0)
    send_own(0, 0)
    send_own(0, 1)

    def relay(j, f, step):
        relay_step(j, f, step)
        if step == 1 and (j, f) in SWAPPED:
            swap(j, f)

    relay(0, 0, 1)
    relay(0, 1, 1)
    attention(1)
    send_own(1, 0)
    send_own(1, 1)
    for f in range(2):
        for step in range(2, n):
            relay(0, f, step)
        relay_cols(0, f)
    for step in range(1, n):
        relay(1, 0, step)
    relay_cols(1, 0)
    early = []
    for f in range(2):
        finish_rows(0, f)
        finish_cols(0, f)
        early += [(f, x, 0, 0), (f, other_x, 0, 0)]
    for step in range(1, n):
        relay(1, 1, step)
        tiles(*early[step - 1])
    relay_cols(1, 1)
    for item in early[n - 1:]:
        tiles(*item)
    for f in range(2):
        finish_cols(1, f)
        for jr, jc in ((0, 1), (1, 0), (1, 1)):
            tiles(f, x, jr, jc)
        tiles(f, other_x, 0, 1)
        finish_rows(1, f)
        for jc in range(2):
            tiles(f, other_x, 1, jc)
    for slot in range(2):
        out_copy(0, x, 0, 0, slot).wait()

    for j in range(2):
        for f in range(2):
            for zs in range(n):
                if (j, f) in SWAPPED:
                    @pl.when(zs != mate)
                    def _():
                        x_copy(j, f, zs).wait_send()

                    @pl.when(zs == z)
                    def _():
                        swap_copy(j, f, zs).wait_send()
                else:
                    x_copy(j, f, zs).wait_send()

                @pl.when((z < n - 1) & (zs <= z))
                def _():
                    up_copy(j, f, zs).wait_send()

                @pl.when((z > 0) & (zs >= z))
                def _():
                    down_copy(j, f, zs).wait_send()

                @pl.when(is_source)
                def _():
                    pair_copy(j, f, zs).wait_send()
                    y_copy(j, f, zs).wait_send()

                @pl.when(far & (core == zs % 2))
                def _():
                    relay_copy(j, f, zs).wait_send()


def fused(query_in, key_in, value_in, out_grads, doc_starts):
    n = lax.axis_size("tokens")
    tok_dev, row_width = query_in.shape
    all_tokens = n * tok_dev
    docs = document_ids(jnp.arange(all_tokens, dtype=jnp.int32), doc_starts)
    dma = pltpu.SemaphoreType.DMA
    hbm = pl.BlockSpec(memory_space=pl.ANY)
    vmem = pl.BlockSpec(memory_space=pltpu.VMEM)
    out = jax.ShapeDtypeStruct((2 * row_width, row_width), F32)
    return tuple(pl.pallas_call(
        fused_kernel,
        out_shape=(out, out),
        in_specs=[hbm] * 4 + [vmem] * 2,
        out_specs=[hbm] * 2,
        scratch_shapes=[
            pltpu.VMEM((2, 4, all_tokens, HEAD_DIM), BF16),
            pltpu.VMEM((2, 2, 2, n, HEAD_DIM, all_tokens), BF16),
            pltpu.VMEM((2, 2, n, HEAD_DIM, all_tokens), BF16),
            pltpu.VMEM((HEAD_DIM, all_tokens), BF16),
            pltpu.VMEM((all_tokens, HEAD_DIM), F32),
            pltpu.VMEM((2, n * HEAD_DIM, n * HEAD_DIM), F32),
            dma((2, 4)), dma((2, 4, n)), dma((2, 4, n)),
            dma((2, 2, 2, n)), dma((2, 2, n)), dma((2, 2, n)), dma((2, 2, n)),
            dma((2, 2, n)), dma((2, 2, n)), dma((2, 2, n)), dma((2, 2, n)),
            dma((2, 2, n)), dma((2,)),
        ],
        compiler_params=pltpu.CompilerParams(
            collective_id=0, has_side_effects=True, vmem_limit_bytes=60 * 1024 * 1024
        ),
    )(query_in, key_in, value_in, out_grads, docs[:, None], docs[None, :]))


def per_device(query_in, key_in, value_in, out_grads, doc_starts):
    n = lax.axis_size("tokens")
    fits = n == 4 and lax.axis_size("heads") == 4 and lax.axis_size("cols") == 2
    if fits and query_in.shape[1] == 2 * n * HEAD_DIM and query_in.shape[0] % BLOCK_Q == 0:
        return fused(query_in, key_in, value_in, out_grads, doc_starts)
    return on_device(query_in, key_in, value_in, out_grads, doc_starts)


def solution(mesh):
    in_specs = (
        P("tokens", ("heads", "cols")),
        P("tokens", ("heads", "cols")),
        P("tokens", ("heads", "cols")),
        P("tokens", ("heads", "cols")),
        P(),
    )
    out_specs = (P("heads", ("tokens", "cols")), P("heads", ("tokens", "cols")))
    return jax.shard_map(
        per_device, mesh=mesh, in_specs=in_specs, out_specs=out_specs, check_vma=False
    )
```

```python
import math

import jax
import jax.numpy as jnp
from jax import lax
from jax.experimental import pallas as pl
from jax.experimental.pallas import tpu as pltpu
from jax.sharding import PartitionSpec as P

HEAD_DIM = 128


MASK_FLOOR = -1e30


def spread(value, axis, source):
    kept = jnp.where(lax.axis_index(axis) == source, value, 0).astype(value.dtype)
    return lax.psum(kept, axis)


def document_ids(positions, doc_starts):
    return jnp.sum((positions[:, None] >= doc_starts[None, :]).astype(jnp.int32), axis=1) - 1


def pair_scores(query_rows, key_rows, query_pos, key_pos, doc_starts):
    head_count = query_rows.shape[1] // HEAD_DIM
    query_heads = query_rows.reshape(query_rows.shape[0], head_count, HEAD_DIM)
    key_heads = key_rows.reshape(key_rows.shape[0], head_count, HEAD_DIM)
    scores = jnp.einsum(
        "qhd,khd->hqk", query_heads, key_heads, preferred_element_type=jnp.float32
    ) * (1.0 / math.sqrt(HEAD_DIM))
    query_docs = document_ids(query_pos, doc_starts)
    key_docs = document_ids(key_pos, doc_starts)
    allowed = query_docs[:, None] == key_docs[None, :]
    return (scores, allowed[None, :, :])


def on_device(query_in, key_in, value_in, out_grads, doc_starts):
    tok_dev, row_width = query_in.shape
    head_count = row_width // HEAD_DIM
    first_pos = lax.axis_index("tokens") * tok_dev
    query_pos = first_pos + jnp.arange(tok_dev, dtype=jnp.int32)
    keys_all, values_all = (
        lax.all_gather(key_in, "tokens", axis=0, tiled=True),
        lax.all_gather(value_in, "tokens", axis=0, tiled=True),
    )
    all_tokens = keys_all.shape[0]
    key_span = min(512, all_tokens)
    block_ids = jnp.arange(all_tokens // key_span, dtype=jnp.int32)

    def block_scores(block_id):
        key_begin = block_id * key_span
        key_rows = lax.dynamic_slice_in_dim(keys_all, key_begin, key_span, 0)
        key_pos = key_begin + jnp.arange(key_span, dtype=jnp.int32)
        scores, allowed = pair_scores(query_in, key_rows, query_pos, key_pos, doc_starts)
        return (key_begin, scores, allowed)

    def gated(block_id, update, running):
        key_begin = block_id * key_span
        return update(running)

    def stats_step(running, block_id):

        def update(state):
            row_peak, row_mass = state
            key_begin, scores, allowed = block_scores(block_id)
            masked = jnp.where(allowed, scores, MASK_FLOOR)
            new_peak = jnp.maximum(row_peak, jnp.max(masked, axis=2))
            new_mass = row_mass * jnp.exp(row_peak - new_peak) + jnp.sum(
                jnp.where(allowed, jnp.exp(masked - new_peak[:, :, None]), 0.0), axis=2
            )
            return (new_peak, new_mass)

        return (gated(block_id, update, running), None)

    initial = (
        jnp.full((head_count, tok_dev), MASK_FLOOR, jnp.float32),
        jnp.zeros((head_count, tok_dev), jnp.float32),
    )
    (row_peak, row_mass), _ = lax.scan(stats_step, initial, block_ids)
    log_total = row_peak + jnp.log(row_mass)

    def value_step(running, block_id):

        def update(state):
            weighted, partials = state
            key_begin, scores, allowed = block_scores(block_id)
            weights = jnp.where(allowed, jnp.exp(scores - log_total[:, :, None]), 0.0).astype(
                jnp.bfloat16
            )
            value_rows = lax.dynamic_slice_in_dim(values_all, key_begin, key_span, 0).reshape(
                key_span, head_count, HEAD_DIM
            )
            weighted = weighted + jnp.einsum(
                "hqk,khd->qhd", weights, value_rows, preferred_element_type=jnp.float32
            )
            return (weighted, partials)

        return (gated(block_id, update, running), None)

    partial_rows = 8
    value_init = (
        jnp.zeros((tok_dev, head_count, HEAD_DIM), jnp.float32),
        jnp.zeros((partial_rows, row_width), jnp.float32),
    )
    (weighted, partials), _ = lax.scan(value_step, value_init, block_ids)
    attended = weighted.reshape(tok_dev, row_width).astype(jnp.bfloat16)
    stats_all = lax.all_gather(log_total.T, "tokens", axis=0, tiled=True)
    query_rows = lax.all_gather(query_in, "tokens", axis=0, tiled=True)
    grad_rows = lax.all_gather(out_grads, "tokens", axis=0, tiled=True)
    piece_rows = query_rows.shape[0]
    piece_pos = jnp.arange(piece_rows, dtype=jnp.int32)

    def update(grad_sum):
        scores, allowed = pair_scores(query_rows, key_in, piece_pos, query_pos, doc_starts)
        weights = jnp.where(allowed, jnp.exp(scores - stats_all.T[:, :, None]), 0.0).astype(
            jnp.bfloat16
        )
        piece_grads = grad_rows.reshape(piece_rows, head_count, HEAD_DIM)
        return jnp.einsum("hqk,qhd->khd", weights, piece_grads, preferred_element_type=jnp.float32)

    summed = update(jnp.zeros((tok_dev, head_count, HEAD_DIM), jnp.float32))
    value_grads = summed.reshape(tok_dev, row_width).astype(jnp.bfloat16)
    token_shards = lax.axis_size("tokens")
    col_shards = lax.axis_size("cols")
    rows_attended, rows_grads = (
        lax.all_gather(attended[None], ("tokens", "cols"), axis=0, tiled=True),
        lax.all_gather(value_grads[None], ("tokens", "cols"), axis=0, tiled=True),
    )
    rows_attended = rows_attended.reshape(token_shards, col_shards, tok_dev, row_width)
    rows_grads = rows_grads.reshape(token_shards, col_shards, tok_dev, row_width)
    own_attended = lax.dynamic_index_in_dim(
        rows_attended, lax.axis_index("cols"), 1, keepdims=False
    )
    own_grads = lax.dynamic_index_in_dim(rows_grads, lax.axis_index("cols"), 1, keepdims=False)
    cols_attended, cols_grads = (
        spread(own_attended, "heads", lax.axis_index("tokens")),
        spread(own_grads, "heads", lax.axis_index("tokens")),
    )
    input_factor = jnp.einsum(
        "acnf,ang->cfg", rows_attended, cols_attended, preferred_element_type=jnp.float32
    )
    grad_factor = jnp.einsum(
        "acnf,ang->cfg", rows_grads, cols_grads, preferred_element_type=jnp.float32
    )
    input_factor = input_factor.reshape(col_shards * row_width, row_width) / all_tokens
    grad_factor = grad_factor.reshape(col_shards * row_width, row_width) / all_tokens
    return (input_factor, grad_factor)


BLOCK_Q = 256
SWAPPED = ((0, 1), (1, 0))
F32 = jnp.float32
BF16 = jnp.bfloat16


def fused_kernel(
    q_ref, k_ref, v_ref, g_ref, dk_ref, dq_ref, out_a, out_g,
    xin, rows, cols, v_t, g_acc, stage,
    own_sem, a2a_send, a2a_recv, row_recv, x_send, up_send, down_send,
    col_recv, pair_send, y_send, relay_send, swap_send, out_sem,
):
    n = lax.axis_size("tokens")
    tok_dev = q_ref.shape[0]
    all_tokens = n * tok_dev
    h = lax.axis_index("heads")
    z = lax.axis_index("tokens")
    x = lax.axis_index("cols")
    y = h // 2
    core = h % 2
    other_x = 1 - x
    pair = y * 2 + (1 - core)
    inputs = (q_ref, k_ref, v_ref, g_ref)

    barrier = pltpu.get_barrier_semaphore()
    for step in range(1, n):
        pl.semaphore_signal(barrier, inc=1, device_id={"tokens": (z + step) % n})
    for step in range(1, 4):
        pl.semaphore_signal(barrier, inc=1, device_id={"heads": (h + step) % 4})
    pl.semaphore_signal(barrier, inc=1, device_id={"cols": other_x})
    pl.semaphore_wait(barrier, n + 3)

    def a2a_copy(j, a, step):
        target = (z + step) % n
        return pltpu.make_async_remote_copy(
            src_ref=inputs[a].at[:, pl.ds(pl.multiple_of((j * n + target) * 128, 128), 128)],
            dst_ref=xin.at[j, a, pl.ds(pl.multiple_of(z * tok_dev, tok_dev), tok_dev), :],
            send_sem=a2a_send.at[j, a, step],
            recv_sem=a2a_recv.at[j, a, step],
            device_id={"tokens": target},
        )

    def own_copy(j, a):
        return pltpu.make_async_copy(
            inputs[a].at[:, pl.ds(pl.multiple_of((j * n + z) * 128, 128), 128)],
            xin.at[j, a, pl.ds(pl.multiple_of(z * tok_dev, tok_dev), tok_dev), :],
            own_sem.at[j, a],
        )

    def send_inputs(j):
        for a in range(4):
            for step in (2, 1, 3):
                a2a_copy(j, a, step).start()
            own_copy(j, a).start()

    def attention(j):
        for a in range(4):
            own_copy(j, a).wait()
            for step in range(1, n):
                a2a_copy(j, a, step).wait()
        if j == 0:
            send_inputs(1)
        v_t[...] = xin[j, 2].astype(F32).T.astype(BF16)
        g_acc[...] = jnp.zeros_like(g_acc)

        def block(ib, carry):
            span = pl.ds(pl.multiple_of(ib * BLOCK_Q, BLOCK_Q), BLOCK_Q)
            s = lax.dot_general(
                xin[j, 1], xin[j, 0, span, :], (((1,), (1,)), ((), ())),
                preferred_element_type=F32,
            ) * (1.0 / math.sqrt(HEAD_DIM))
            s = jnp.where(dk_ref[...] == dq_ref[:, span], s, MASK_FLOOR)
            e = jnp.exp(s - jnp.max(s, axis=0, keepdims=True))
            p = (e * (1.0 / jnp.sum(e, axis=0, keepdims=True))).astype(BF16)
            att = jnp.dot(v_t[...], p, preferred_element_type=F32)
            rows[j, 0, x, z, :, span] = att.astype(BF16)
            g_acc[...] += jnp.dot(p, xin[j, 3, span, :], preferred_element_type=F32)
            return carry

        lax.fori_loop(0, all_tokens // BLOCK_Q, block, 0)
        rows[j, 1, x, z] = g_acc[...].T.astype(BF16)

    def row_copy(j, f, xs, zs, send, device):
        piece = rows.at[j, f, xs, zs]
        return pltpu.make_async_remote_copy(
            src_ref=piece, dst_ref=piece, send_sem=send.at[j, f, zs],
            recv_sem=row_recv.at[j, f, xs, zs], device_id=device,
        )

    def x_copy(j, f, zs):
        return row_copy(j, f, x, zs, x_send, {"cols": other_x})

    def up_copy(j, f, zs):
        return row_copy(j, f, x, zs, up_send, {"tokens": (z + 1) % n})

    def down_copy(j, f, zs):
        return row_copy(j, f, x, zs, down_send, {"tokens": (z + n - 1) % n})

    def col_copy(j, f, zs, source, send, device):
        return pltpu.make_async_remote_copy(
            src_ref=source, dst_ref=cols.at[j, f, zs], send_sem=send.at[j, f, zs],
            recv_sem=col_recv.at[j, f, zs], device_id={"heads": device},
        )

    def pair_copy(j, f, zs):
        return col_copy(j, f, zs, rows.at[j, f, x, zs], pair_send, pair)

    def y_copy(j, f, zs):
        return col_copy(j, f, zs, rows.at[j, f, x, zs], y_send, (1 - y) * 2 + zs % 2)

    def relay_copy(j, f, zs):
        return col_copy(j, f, zs, cols.at[j, f, zs], relay_send, pair)

    mate = z + 1 - 2 * (z % 2)

    def swap_copy(j, f, zs):
        return row_copy(j, f, other_x, zs, swap_send, {"tokens": mate})

    def swap(j, f):
        x_copy_in = row_copy(j, f, other_x, z, x_send, {"cols": other_x})
        x_copy_in.wait_recv()
        swap_copy(j, f, z).start()

    def relay_x(j, f, zs):
        if (j, f) in SWAPPED:
            @pl.when(zs != mate)
            def _():
                x_copy(j, f, zs).start()
        else:
            x_copy(j, f, zs).start()

    is_source = h == z
    far = y != z // 2

    def feed_cols(j, f, zs):
        @pl.when(is_source)
        def _():
            pair_copy(j, f, zs).start()
            y_copy(j, f, zs).start()

    def send_own(j, f):
        @pl.when(z < n - 1)
        def _():
            up_copy(j, f, z).start()

        @pl.when(z > 0)
        def _():
            down_copy(j, f, z).start()

        x_copy(j, f, z).start()
        feed_cols(j, f, z)

    def relay_step(j, f, step):
        @pl.when(z >= step)
        def _():
            zs = z - step
            x_copy(j, f, zs).wait_recv()

            @pl.when(z < n - 1)
            def _():
                up_copy(j, f, zs).start()

            relay_x(j, f, zs)
            feed_cols(j, f, zs)

        @pl.when(z + step < n)
        def _():
            zs = z + step
            x_copy(j, f, zs).wait_recv()

            @pl.when(z > 0)
            def _():
                down_copy(j, f, zs).start()

            relay_x(j, f, zs)
            feed_cols(j, f, zs)

    def relay_cols(j, f):
        for zs in range(n):
            @pl.when(far & (core == zs % 2))
            def _():
                relay_copy(j, f, zs).wait_recv()
                relay_copy(j, f, zs).start()

    def finish_rows(j, f):
        def one(zs, carry):
            waiting = row_copy(j, f, other_x, zs, x_send, {"cols": other_x})
            if (j, f) in SWAPPED:
                @pl.when(zs != z)
                def _():
                    waiting.wait_recv()
            else:
                waiting.wait_recv()
            return carry

        lax.fori_loop(0, n, one, 0)

    def finish_cols(j, f):
        for zs in range(n):
            @pl.when((h != z) & jnp.logical_not(far & (core == zs % 2)))
            def _():
                relay_copy(j, f, zs).wait_recv()

        @pl.when(is_source)
        def _():
            def move(zs, carry):
                cols[j, f, zs] = rows[j, f, x, zs]
                return carry

            lax.fori_loop(0, n, move, 0)

    used = [0]
    span_rows = n * 128

    def out_copy(f, xs, jr, jc, slot):
        target = (out_a, out_g)[f]
        return pltpu.make_async_copy(
            stage.at[slot],
            target.at[
                pl.ds(pl.multiple_of(xs * (2 * span_rows) + jr * span_rows, span_rows), span_rows),
                pl.ds(jc * span_rows, span_rows),
            ],
            out_sem.at[slot],
        )

    def tiles(f, xs, jr, jc):
        slot = used[0] % 2
        if used[0] >= 2:
            out_copy(f, xs, jr, jc, slot).wait()
        used[0] += 1

        def part(m, carry):
            left = rows[jr, f, xs, pl.ds(2 * m, 2)].reshape(256, all_tokens)
            right = cols[jc, f].reshape(span_rows, all_tokens)
            stage[slot, pl.ds(pl.multiple_of(m * 256, 256), 256), :] = lax.dot_general(
                left, right, (((1,), (1,)), ((), ())), preferred_element_type=F32
            ) * (1.0 / all_tokens)
            return carry

        lax.fori_loop(0, n // 2, part, 0)
        out_copy(f, xs, jr, jc, slot).start()

    send_inputs(0)
    attention(0)
    send_own(0, 0)
    send_own(0, 1)

    def relay(j, f, step):
        relay_step(j, f, step)
        if step == 1 and (j, f) in SWAPPED:
            swap(j, f)

    relay(0, 0, 1)
    relay(0, 1, 1)
    attention(1)
    send_own(1, 0)
    send_own(1, 1)
    for step in range(2, n):
        relay(0, 0, step)
        relay(0, 1, step)
        relay(1, 0, step - 1)
        relay(1, 1, step - 1)
    relay_cols(0, 0)
    relay_cols(0, 1)
    early = []
    for f in range(2):
        finish_rows(0, f)
        finish_cols(0, f)
        early += [(f, x, 0, 0), (f, other_x, 0, 0)]
    for f in range(2):
        tiles(*early[f])
        relay(1, f, n - 1)
    relay_cols(1, 0)
    relay_cols(1, 1)
    for item in early[2:]:
        tiles(*item)
    for f in range(2):
        finish_cols(1, f)
        for jr, jc in ((0, 1), (1, 0), (1, 1)):
            tiles(f, x, jr, jc)
        tiles(f, other_x, 0, 1)
        finish_rows(1, f)
        for jc in range(2):
            tiles(f, other_x, 1, jc)
    for slot in range(2):
        out_copy(0, x, 0, 0, slot).wait()

    for j in range(2):
        for f in range(2):
            for zs in range(n):
                if (j, f) in SWAPPED:
                    @pl.when(zs != mate)
                    def _():
                        x_copy(j, f, zs).wait_send()

                    @pl.when(zs == z)
                    def _():
                        swap_copy(j, f, zs).wait_send()
                else:
                    x_copy(j, f, zs).wait_send()

                @pl.when((z < n - 1) & (zs <= z))
                def _():
                    up_copy(j, f, zs).wait_send()

                @pl.when((z > 0) & (zs >= z))
                def _():
                    down_copy(j, f, zs).wait_send()

                @pl.when(is_source)
                def _():
                    pair_copy(j, f, zs).wait_send()
                    y_copy(j, f, zs).wait_send()

                @pl.when(far & (core == zs % 2))
                def _():
                    relay_copy(j, f, zs).wait_send()


def fused(query_in, key_in, value_in, out_grads, doc_starts):
    n = lax.axis_size("tokens")
    tok_dev, row_width = query_in.shape
    all_tokens = n * tok_dev
    docs = document_ids(jnp.arange(all_tokens, dtype=jnp.int32), doc_starts)
    dma = pltpu.SemaphoreType.DMA
    hbm = pl.BlockSpec(memory_space=pl.ANY)
    vmem = pl.BlockSpec(memory_space=pltpu.VMEM)
    out = jax.ShapeDtypeStruct((2 * row_width, row_width), F32)
    return tuple(pl.pallas_call(
        fused_kernel,
        out_shape=(out, out),
        in_specs=[hbm] * 4 + [vmem] * 2,
        out_specs=[hbm] * 2,
        scratch_shapes=[
            pltpu.VMEM((2, 4, all_tokens, HEAD_DIM), BF16),
            pltpu.VMEM((2, 2, 2, n, HEAD_DIM, all_tokens), BF16),
            pltpu.VMEM((2, 2, n, HEAD_DIM, all_tokens), BF16),
            pltpu.VMEM((HEAD_DIM, all_tokens), BF16),
            pltpu.VMEM((all_tokens, HEAD_DIM), F32),
            pltpu.VMEM((2, n * HEAD_DIM, n * HEAD_DIM), F32),
            dma((2, 4)), dma((2, 4, n)), dma((2, 4, n)),
            dma((2, 2, 2, n)), dma((2, 2, n)), dma((2, 2, n)), dma((2, 2, n)),
            dma((2, 2, n)), dma((2, 2, n)), dma((2, 2, n)), dma((2, 2, n)),
            dma((2, 2, n)), dma((2,)),
        ],
        compiler_params=pltpu.CompilerParams(
            collective_id=0, has_side_effects=True, vmem_limit_bytes=60 * 1024 * 1024
        ),
    )(query_in, key_in, value_in, out_grads, docs[:, None], docs[None, :]))


def per_device(query_in, key_in, value_in, out_grads, doc_starts):
    n = lax.axis_size("tokens")
    fits = n == 4 and lax.axis_size("heads") == 4 and lax.axis_size("cols") == 2
    if fits and query_in.shape[1] == 2 * n * HEAD_DIM and query_in.shape[0] % BLOCK_Q == 0:
        return fused(query_in, key_in, value_in, out_grads, doc_starts)
    return on_device(query_in, key_in, value_in, out_grads, doc_starts)


def solution(mesh):
    in_specs = (
        P("tokens", ("heads", "cols")),
        P("tokens", ("heads", "cols")),
        P("tokens", ("heads", "cols")),
        P("tokens", ("heads", "cols")),
        P(),
    )
    out_specs = (P("heads", ("tokens", "cols")), P("heads", ("tokens", "cols")))
    return jax.shard_map(
        per_device, mesh=mesh, in_specs=in_specs, out_specs=out_specs, check_vma=False
    )
```
